32 devices in a mesh: gx: 4 (over z), gy: 2 (over y), gz: 4 (over x, core).
Axes of the slice: x: 2, y: 2, z: 4, core: 2. Of those that a mesh axis runs over, the one named last changes fastest.
Arguments:
- positions: float32 [3, 8, 4, 32, 128], P(None, 'gx', 'gy', 'gz'), may hold values from 0 to 1
- shield: float32 [8, 4, 32, 128], P('gx', 'gy', 'gz'), may hold values from 0.3 to 1
- width: float32 [8, 4, 32, 128], P('gx', 'gy', 'gz'), may hold values from 0.5 to 2
- hardness: float32 [8, 4, 32, 128], P('gx', 'gy', 'gz'), may hold values from 0.5 to 2
- softness: float32 [8, 4, 32, 128], P('gx', 'gy', 'gz'), may hold values from 0.5 to 2
- coupling: float32 [8, 4, 32, 128], P('gx', 'gy', 'gz'), may hold values from -0.45 to 0.45
- pair_bits: int32 [8, 4, 32], P('gx', 'gy', 'gz'), may hold values from 8192 to 134217727, as said below
- right_side: float32 [4, 8, 4, 32, 128], P(None, 'gx', 'gy', 'gz'), may hold values from -7 to 7
Outputs:
- solution: float32 [4, 8, 4, 32, 128], P(None, 'gx', 'gy', 'gz')
- residual: float32 [4, 8, 4, 32, 128], P(None, 'gx', 'gy', 'gz')
The draws below stay inside these ranges and needn't reach their ends.
Inputs may be any that keep to these rules, and one draw needn't show every extreme that they name: `pair_bits`: bit k of a tile's word stands for the offset with code k as in the reference program; bit 13 is always 1, bits 27 and up are 0, a bit is 0 where the offset leaves the grid, and the lists are symmetric: bit k of tile t equals bit 26 - k of the tile at t plus that offset.
All inputs are finite; a program needn't handle non-finite values.
Results may differ from the reference program's by a relative error of at most 0.0018.
Values sent between devices are 32-bit elements; how exact they have to be, the bound alone decides.
A program may use at most 128 MiB of HBM per device.

```python
import math
import jax
import jax.numpy as jnp
from jax import lax

TILE = 128
ITERS = 3
NTX = 8
NTY = 4
NTZ = 32


def draw_pair_bits(key, part):
    forward_bits = jax.random.randint(key, (NTX, NTY, NTZ, 13), 0, 2).astype(jnp.int32)
    padded_bits = jnp.pad(forward_bits, ((1, 1), (1, 1), (1, 1), (0, 0)))
    index_first = lax.broadcasted_iota(jnp.int32, (NTX, NTY, NTZ), 0)
    index_second = lax.broadcasted_iota(jnp.int32, (NTX, NTY, NTZ), 1)
    index_third = lax.broadcasted_iota(jnp.int32, (NTX, NTY, NTZ), 2)
    packed = jnp.full((NTX, NTY, NTZ), 1 << 13, jnp.int32)
    for offset_code in range(27):
        shift_first = offset_code // 9 - 1
        shift_second = offset_code // 3 % 3 - 1
        shift_third = offset_code % 3 - 1
        if offset_code > 13:
            inside = (index_first + shift_first >= 0) & (index_first + shift_first < NTX)
            inside = inside & (index_second + shift_second >= 0) & (index_second + shift_second < NTY)
            inside = inside & (index_third + shift_third >= 0) & (index_third + shift_third < NTZ)
            chosen = jnp.where(inside, forward_bits[:, :, :, offset_code - 14], 0)
            packed = packed + chosen * (1 << offset_code)
        elif offset_code < 13:
            chosen = padded_bits[1 + shift_first:1 + shift_first + NTX, 1 + shift_second:1 + shift_second + NTY, 1 + shift_third:1 + shift_third + NTZ, 12 - offset_code]
            packed = packed + chosen * (1 << offset_code)
    return packed


def draw_right_side(key, part):
    rough_key = jax.random.fold_in(key, 11)
    sign_key = jax.random.fold_in(key, 12)
    wave_key = jax.random.fold_in(key, 13)
    phase_key = jax.random.fold_in(key, 14)
    shape = (4, NTX, NTY, NTZ, TILE)
    rough = jnp.clip(jax.random.normal(rough_key, shape, jnp.float32), -4.0, 4.0)
    signs = jnp.where(jax.random.bernoulli(sign_key, 0.5, (4,)), 1.0, -1.0).astype(jnp.float32)
    waves = jax.random.randint(wave_key, (4, 3), 1, 3).astype(jnp.float32)
    phases = jax.random.uniform(phase_key, (4,), jnp.float32, -math.pi, math.pi)
    coord_first = (lax.broadcasted_iota(jnp.float32, (NTX, NTY, NTZ), 0) + 0.5) / NTX
    coord_second = (lax.broadcasted_iota(jnp.float32, (NTX, NTY, NTZ), 1) + 0.5) / NTY
    coord_third = (lax.broadcasted_iota(jnp.float32, (NTX, NTY, NTZ), 2) + 0.5) / NTZ
    phase_field = waves[:, 0, None, None, None] * coord_first[None] + waves[:, 1, None, None, None] * coord_second[None] + waves[:, 2, None, None, None] * coord_third[None]
    phase_field = 2.0 * math.pi * phase_field + phases[:, None, None, None]
    smooth = signs[:, None, None, None] * (1.0 + 0.5 * jnp.cos(phase_field))
    return (rough + smooth[..., None]).astype(jnp.float32)


def level_of(own_key, dims, pieces, low, top_value):
    def one(position, parts):
        steps = jax.random.uniform(jax.random.fold_in(jax.random.fold_in(own_key, 6), position), (parts,), jnp.float32, low / len(pieces), top_value / len(pieces))
        return jnp.repeat(jnp.exp(steps), dims[position] // parts).reshape((-1,) + (1,) * (len(dims) - position - 1))

    factor_of = one(*pieces[0])
    for cut in pieces[1:]:
        factor_of = factor_of * one(*cut)
    return factor_of


def setup_inputs(seed: int = 0) -> dict:
    key_of = jax.random.split(jax.random.key(seed), 9)
    positions = jnp.clip(1.0 * jax.random.uniform(key_of[0], (3, NTX, NTY, NTZ, TILE), jnp.float32) ** level_of(key_of[0], (3, NTX, NTY, NTZ, TILE), ((1, 4), (2, 2), (3, 4)), -0.2, 0.2), 0.0, 1.0)
    shield = jnp.clip(jnp.exp(math.log(1.0) - 1.2039728 * jax.random.uniform(key_of[1], (NTX, NTY, NTZ, TILE), jnp.float32) ** level_of(key_of[1], (NTX, NTY, NTZ, TILE), ((0, 4), (1, 2), (2, 4)), -0.2, 0.2)), 0.3, 1.0)
    width = jnp.clip(jnp.exp(math.log(2.0) - 1.3862944 * jax.random.uniform(key_of[2], (NTX, NTY, NTZ, TILE), jnp.float32) ** level_of(key_of[2], (NTX, NTY, NTZ, TILE), ((0, 4), (1, 2), (2, 4)), -0.2, 0.2)), 0.5, 2.0)
    hardness = jnp.clip(jnp.exp(math.log(2.0) - 1.3862944 * jax.random.uniform(key_of[3], (NTX, NTY, NTZ, TILE), jnp.float32) ** level_of(key_of[3], (NTX, NTY, NTZ, TILE), ((0, 4), (1, 2), (2, 4)), -0.2, 0.2)), 0.5, 2.0)
    softness = jnp.clip(jnp.exp(math.log(2.0) - 1.3862944 * jax.random.uniform(key_of[4], (NTX, NTY, NTZ, TILE), jnp.float32) ** level_of(key_of[4], (NTX, NTY, NTZ, TILE), ((0, 4), (1, 2), (2, 4)), -0.2, 0.2)), 0.5, 2.0)
    coupling = jnp.clip(jax.random.uniform(key_of[5], (NTX, NTY, NTZ, TILE), jnp.float32, -0.45, 0.45) * level_of(key_of[5], (NTX, NTY, NTZ, TILE), ((0, 4), (1, 2), (2, 4)), -0.4, 0.0), -0.45, 0.45)
    pair_bits = draw_pair_bits(jax.random.fold_in(key_of[8], 71), 0)
    right_side = draw_right_side(jax.random.fold_in(key_of[8], 71), 0)
    return dict(positions=positions, shield=shield, width=width, hardness=hardness, softness=softness, coupling=coupling, pair_bits=pair_bits, right_side=right_side)


coulomb_scale = 0.002
response_scale = 0.003

def index_tuple(values):
    return tuple((jnp.asarray(value).astype(jnp.int32) for value in values))

def pair_terms(own_params, partner, offset_code, own_bits):
    shift_first = (offset_code // 9 - 1).astype(jnp.float32)
    shift_second = (offset_code // 3 % 3 - 1).astype(jnp.float32)
    shift_third = (offset_code % 3 - 1).astype(jnp.float32)

    def separation(column, shift):
        return shift + (partner[column][:, None, :] - own_params[column][:, :, None])
    first = separation(0, shift_first)
    second = separation(1, shift_second)
    third = separation(2, shift_third)
    distance = first * first + second * second + third * third
    coulomb = coulomb_scale * lax.rsqrt(distance + own_params[3][:, :, None] * partner[3][:, None, :])
    response = response_scale * jnp.exp(-distance / (own_params[4][:, :, None] + partner[4][:, None, :]))
    listed = jnp.right_shift(own_bits, offset_code) & 1 > 0
    tile_size = own_params.shape[2]
    diagonal_mask = lax.broadcasted_iota(jnp.int32, (tile_size, tile_size), 0) == lax.broadcasted_iota(jnp.int32, (tile_size, tile_size), 1)
    kept = listed[:, None, None] & jnp.logical_not(diagonal_mask[None] & (offset_code == 13))
    empty_pair = jnp.zeros_like(distance)
    return (jnp.where(kept, coulomb, empty_pair).astype(jnp.bfloat16), jnp.where(kept, response, empty_pair).astype(jnp.bfloat16))

def inner(vector, other_vector):
    return lax.optimization_barrier(jnp.sum((vector * other_vector).reshape(2, 2, -1), axis=(0, 2)))

def widen(scalars):
    return jnp.concatenate([scalars, scalars]).reshape(4, 1, 1, 1, 1)

def reference(positions, shield, width, hardness, softness, coupling, pair_bits, right_side):
    tiles_x, tiles_y, tiles_z, tile_size = hardness.shape
    params = jnp.concatenate([positions, shield[None], width[None]], axis=0)
    params_pad = jnp.pad(params, ((0, 0), (1, 1), (1, 1), (1, 1), (0, 0)))
    plane = tiles_y * tiles_z

    def operate(vector):
        vector_pad = jnp.pad(vector, ((0, 0), (1, 1), (1, 1), (1, 1), (0, 0)))

        def slab_terms(slab_index):
            slab_index = slab_index.astype(jnp.int32)
            own_params = lax.dynamic_slice(params_pad, index_tuple((0, slab_index + 1, 1, 1, 0)), (5, 1, tiles_y, tiles_z, tile_size)).reshape(5, plane, tile_size)
            own_bits = lax.dynamic_slice(pair_bits, index_tuple((slab_index, 0, 0)), (1, tiles_y, tiles_z)).reshape(plane)

            def visit(offset_code, carry):
                row_coulomb, row_response, pair_charge, pair_potential = carry
                offset_code = offset_code.astype(jnp.int32)
                start = index_tuple((0, slab_index + offset_code // 9, offset_code // 3 % 3, offset_code % 3, 0))
                partner = lax.dynamic_slice(params_pad, start, (5, 1, tiles_y, tiles_z, tile_size)).reshape(5, plane, tile_size)
                neighbour = lax.dynamic_slice(vector_pad, start, (4, 1, tiles_y, tiles_z, tile_size)).reshape(4, plane, tile_size)
                coulomb, response = pair_terms(own_params, partner, offset_code, own_bits)
                coulomb = coulomb.astype(jnp.float32)
                response = response.astype(jnp.float32)
                row_coulomb = row_coulomb + lax.optimization_barrier(jnp.sum(coulomb, axis=2))
                row_response = row_response + lax.optimization_barrier(jnp.sum(response, axis=2))
                pair_charge = pair_charge + jnp.einsum('tij,ftj->fti', coulomb, neighbour[:2], precision=lax.Precision.HIGHEST)
                pair_potential = pair_potential + jnp.einsum('tij,ftj->fti', response, neighbour[2:], precision=lax.Precision.HIGHEST)
                return (row_coulomb, row_response, pair_charge, pair_potential)
            flat_zeros = jnp.zeros((plane, tile_size), jnp.float32)
            pair_zeros = jnp.zeros((2, plane, tile_size), jnp.float32)
            return lax.fori_loop(0, 27, visit, (flat_zeros, flat_zeros, pair_zeros, pair_zeros))
        row_coulomb, row_response, pair_charge, pair_potential = lax.map(slab_terms, jnp.arange(tiles_x, dtype=jnp.int32))
        grid = (tiles_x, tiles_y, tiles_z, tile_size)
        row_coulomb = row_coulomb.reshape(grid)
        row_response = row_response.reshape(grid)
        pair_charge = pair_charge.transpose(1, 0, 2, 3).reshape((2,) + grid)
        pair_potential = pair_potential.transpose(1, 0, 2, 3).reshape((2,) + grid)
        image_charge = (hardness + row_coulomb) * vector[:2] + pair_charge + coupling * vector[2:]
        image_potential = (softness + row_response) * vector[2:] - pair_potential + coupling * vector[:2]
        return jnp.concatenate([image_charge, image_potential], axis=0)
    solution = jnp.zeros_like(right_side)
    remainder = right_side
    direction = right_side
    norm_now = inner(remainder, remainder)
    for iteration in range(ITERS):
        applied = operate(direction)
        step_size = norm_now / inner(direction, applied)
        solution = solution + widen(step_size) * direction
        remainder = remainder - widen(step_size) * applied
        norm_next = inner(remainder, remainder)
        direction = remainder + widen(norm_next / norm_now) * direction
        norm_now = norm_next
    residual = right_side - operate(solution)
    return (solution, residual)
```

```python
import functools
import itertools

import jax
import jax.numpy as jnp
from jax import lax
from jax.experimental import pallas as pl
from jax.experimental.pallas import tpu as pltpu
from jax.sharding import PartitionSpec as P

ITERS = 3
AXES = ("gx", "gy", "gz")
DIRECTIONS = [d for d in itertools.product((-1, 0, 1), repeat=3) if d != (0, 0, 0)]

coulomb_scale = 0.002
response_scale = 0.003


def sides(step, count, unit):
    if step < 0:
        return pl.ds(unit, unit), pl.ds((count + 1) * unit, unit)
    if step > 0:
        return pl.ds(count * unit, unit), pl.ds(0, unit)
    return pl.ds(unit, count * unit), pl.ds(unit, count * unit)


def kernel(
    counts, extent, tile,
    bits_ref, params_ref, rhs_ref, aux_ref, sol_ref, res_ref,
    store, param_pad, rem_pad, along_pad, ghosts, lhs, columns, diag, direction, sums, parts,
    halo_send, halo_recv, sum_send, sum_recv,
):
    tx, ty, tz = extent
    me = [lax.axis_index(axis) for axis in AXES]

    def exists(d):
        ok = None
        for m, step, count in zip(me, d, counts):
            if step:
                here = (m + step >= 0) & (m + step < count)
                ok = here if ok is None else ok & here
        return ok

    def halo_copy(ref, slot, index, d):
        pairs = [sides(s, n, u) for s, n, u in zip(d, extent, (1, 1, tile))]
        source = (pairs[0][0], pairs[1][0], slice(None), pairs[2][0])
        target = (pairs[0][1], pairs[1][1], slice(None), pairs[2][1])
        return pltpu.make_async_remote_copy(
            src_ref=ref.at[source],
            dst_ref=ref.at[target],
            send_sem=halo_send.at[slot, index],
            recv_sem=halo_recv.at[slot, index],
            device_id=tuple(m + s for m, s in zip(me, d)),
            device_id_type=pl.DeviceIdType.MESH,
        )

    def halo_start(ref, slot, fill):
        for index, d in enumerate(DIRECTIONS):
            there = exists(d)

            @pl.when(there)
            def _():
                halo_copy(ref, slot, index, d).start()

            back = tuple(-s for s in d)
            strips = [sides(s, n, u)[1] for s, n, u in zip(back, extent, (1, 1, tile))]

            @pl.when(jnp.logical_not(there))
            def _():
                region = (strips[0], strips[1], slice(None), strips[2])
                ref[region] = jnp.full(ref.at[region].shape, fill, jnp.float32)

    def halo_wait(ref, slot):
        for index, d in enumerate(DIRECTIONS):
            @pl.when(exists(d))
            def _():
                halo_copy(ref, slot, index, d).wait_send()

            back = tuple(-s for s in d)

            @pl.when(exists(back))
            def _():
                halo_copy(ref, slot, index, d).wait_recv()

    def sum_copies(slot, stage):
        count = counts[stage]
        copies = []
        for j in range(1, count):
            target = list(me)
            target[stage] = lax.rem(me[stage] + j, count)
            copies.append(
                pltpu.make_async_remote_copy(
                    src_ref=sums.at[slot, stage],
                    dst_ref=parts.at[slot, stage, me[stage]],
                    send_sem=sum_send.at[slot, stage, j],
                    recv_sem=sum_recv.at[slot, stage, j],
                    device_id=tuple(target),
                    device_id_type=pl.DeviceIdType.MESH,
                )
            )
        return copies

    def reduced(slot, value):
        for stage in (2, 1, 0):
            if counts[stage] == 1:
                continue
            sums[slot, stage] = value
            parts[slot, stage, me[stage]] = value
            copies = sum_copies(slot, stage)
            for copy in copies:
                copy.start()
            for copy in copies:
                copy.wait()
            value = parts[slot, stage, 0]
            for k in range(1, counts[stage]):
                value = value + parts[slot, stage, k]
        total = jnp.sum(value, axis=1, keepdims=True)
        norm, product = total[:4], total[4:]

        def both(x):
            return x + jnp.concatenate([x[2:4], x[0:2]], axis=0)

        return both(norm), both(product)

    inside = pl.ds(tile, tz * tile)
    for a in range(tx):
        for b in range(ty):
            param_pad[a + 1, b + 1, :, inside] = params_ref[a, b]
            rem_pad[a + 1, b + 1, :, inside] = rhs_ref[a, b]
    halo_start(param_pad, 0, 1.0)
    halo_start(rem_pad, 1, 0.0)

    def source_block(ap, bp, p, widths):
        start = pl.multiple_of(p * tile, tile)
        turned = param_pad[ap, bp, :, pl.ds(start, tile)].T
        for m in range(5):
            columns[m] = jnp.broadcast_to(turned[:, m : m + 1], (tile, tile))

        def visit(a, b):
            for c in widths:
                o = (ap - 1 - a, bp - 1 - b, p - 1 - c)
                code = 9 * (o[0] + 1) + 3 * (o[1] + 1) + (o[2] + 1)
                t = (a * ty + b) * tz + c
                listed = jnp.right_shift(bits_ref[t], code) & 1
                own = param_pad[
                    a + 1, b + 1, :, pl.ds(pl.multiple_of((c + 1) * tile, tile), tile)
                ]
                distance = None
                for m in range(3):
                    gap = columns[m] - (own[m : m + 1] - o[m].astype(jnp.float32))
                    distance = gap * gap if distance is None else distance + gap * gap
                listed = listed.astype(jnp.float32)
                coulomb = lax.rsqrt(distance + columns[3] * own[3:4]) * (coulomb_scale * listed)
                response = jnp.exp(-(distance / (columns[4] + own[4:5]))) * (
                    response_scale * listed
                )
                rows = pl.ds(pl.multiple_of(code * tile, tile), tile)
                store[t, rows, 0:tile] = coulomb.astype(jnp.bfloat16)
                store[t, rows, tile : 2 * tile] = response.astype(jnp.bfloat16)

        def over_a(a, carry):
            def over_b(b, inner_carry):
                visit(a, b)
                return inner_carry

            return lax.fori_loop(
                jnp.maximum(bp - 2, 0), jnp.minimum(bp, ty - 1) + 1, over_b, carry
            )

        lax.fori_loop(jnp.maximum(ap - 2, 0), jnp.minimum(ap, tx - 1) + 1, over_a, 0)

    def edge_sources(ap, bp, first, second, wide):
        def step(s, carry):
            p = first + s * (second - first)
            base = s * (tz - wide)
            source_block(ap, bp, p, [base + w for w in range(wide)])
            return carry

        lax.fori_loop(0, 2, step, 0)

    def middle_sources(ap, bp):
        def step(p, carry):
            source_block(ap, bp, p, [p - 2, p - 1, p])
            return carry

        lax.fori_loop(2, tz, step, 0)

    def own_rows(body):
        def over(q, carry):
            body(1 + q // ty, 1 + q % ty)
            return carry

        lax.fori_loop(0, tx * ty, over, 0)

    def build_own(ap, bp):
        middle_sources(ap, bp)
        edge_sources(ap, bp, 1, tz, 2)

    own_rows(build_own)

    same = lax.broadcasted_iota(jnp.int32, (tile, 2 * tile), 0) == (
        lax.broadcasted_iota(jnp.int32, (tile, 2 * tile), 1) % tile
    )

    def clear(t, carry):
        rows = pl.ds(13 * tile, tile)
        block = store[t, rows, :].astype(jnp.float32)
        store[t, rows, :] = jnp.where(same, 0.0, block).astype(jnp.bfloat16)
        return carry

    lax.fori_loop(0, tx * ty * tz, clear, 0)

    halo_wait(param_pad, 0)

    own_rows(lambda ap, bp: edge_sources(ap, bp, 0, tz + 1, 1))

    def ghost_row(q, carry):
        ap = q // (ty + 2)
        bp = q % (ty + 2)
        own = (ap >= 1) & (ap <= tx) & (bp >= 1) & (bp <= ty)

        @pl.when(jnp.logical_not(own))
        def _():
            middle_sources(ap, bp)
            edge_sources(ap, bp, 1, tz, 2)
            edge_sources(ap, bp, 0, tz + 1, 1)

        return carry

    lax.fori_loop(0, (tx + 2) * (ty + 2), ghost_row, 0)
    halo_wait(rem_pad, 1)

    charge_rows = lax.broadcasted_iota(jnp.int32, (4, tile), 0) < 2

    def operate(out, first):
        def split(q, carry):
            ap = q // (ty + 2)
            bp = q % (ty + 2)
            value = rem_pad[ap, bp]
            upper = value.astype(jnp.bfloat16).astype(jnp.float32)
            lower = value - upper
            ones = jnp.ones((8, value.shape[1]), jnp.float32)
            lhs[ap, bp] = jnp.concatenate([upper, lower, ones], axis=0).astype(jnp.bfloat16)
            return carry

        lax.fori_loop(0, (tx + 2) * (ty + 2), split, 0)

        def one(t, carry):
            norm, product = carry
            a = t // (ty * tz)
            b = t // tz % ty
            c = t % tz
            window = pl.ds(pl.multiple_of(c * tile, tile), 3 * tile)
            rows = jnp.concatenate(
                [lhs[a + i, b + j, :, window] for i in range(3) for j in range(3)], axis=1
            )
            got = jnp.dot(rows, store[t], preferred_element_type=jnp.float32)
            pair = got[0:4] + got[4:8]
            pair = jnp.where(charge_rows, pair[:, :tile], -pair[:, tile:])
            here = pl.ds(pl.multiple_of(c * tile, tile), tile)
            there = pl.ds(pl.multiple_of((c + 1) * tile, tile), tile)
            if first:
                row_sums = jnp.where(charge_rows, got[8:12, :tile], got[8:12, tile:])
                own = aux_ref[a, b, :, here]
                diag[a, b, :, here] = row_sums + jnp.where(charge_rows, own[0:1], own[1:2])
            vector = rem_pad[a + 1, b + 1, :, there]
            swapped = jnp.concatenate([vector[2:4], vector[0:2]], axis=0)
            link = aux_ref[a, b, 2:3, here]
            image = diag[a, b, :, here] * vector + pair + link * swapped
            out[a + 1, b + 1, :, there] = image
            return (norm + vector * vector, product + vector * image)

        zero = jnp.zeros((4, tile), jnp.float32)
        norm, product = lax.fori_loop(0, tx * ty * tz, one, (zero, zero), unroll=2)
        return jnp.concatenate([norm, product], axis=0)

    interior = (pl.ds(1, tx), pl.ds(1, ty), slice(None), inside)
    norm_now = step_size = None
    for iteration in range(ITERS):
        last = iteration + 1 == ITERS
        image = ghosts.at[iteration]
        partial = operate(image, iteration == 0)
        if not last:
            halo_start(image, 2 + iteration, 0.0)
        norm_next, product = reduced(iteration, partial)
        if not last:
            halo_wait(image, 2 + iteration)
        if iteration == 0:
            beta = None
            step_size = norm_next / product
        else:
            beta = norm_next / norm_now
            step_size = norm_next / (product - beta * norm_next / step_size)
        norm_now = norm_next
        for a in range(tx):
            for b in range(ty):
                along_dir = rem_pad[a + 1, b + 1, :, inside]
                if beta is not None:
                    along_dir = along_dir + beta * direction[a, b]
                direction[a, b] = along_dir
                moved = step_size * along_dir
                sol_ref[a, b] = moved if beta is None else sol_ref[a, b] + moved
        if last:
            for a in range(tx):
                for b in range(ty):
                    along = image[a + 1, b + 1, :, inside] + beta * along_pad[a + 1, b + 1, :, inside]
                    res_ref[a, b] = rem_pad[a + 1, b + 1, :, inside] - step_size * along
        else:
            for a in range(tx + 2):
                for b in range(ty + 2):
                    along = image[a, b]
                    if beta is not None:
                        along = along + beta * along_pad[a, b]
                    along_pad[a, b] = along
                    rem_pad[a, b] = rem_pad[a, b] - step_size * along


def on_device(counts, positions, shield, width, hardness, softness, coupling, pair_bits, right_side):
    tx, ty, tz, tile = hardness.shape
    blank = jnp.ones_like(width)

    def rows(fields):
        stacked = jnp.stack(fields, axis=2)
        return stacked.reshape(tx, ty, len(fields), tz * tile)

    params = rows([positions[0], positions[1], positions[2], shield, width, blank, blank, blank])
    aux = rows([hardness, softness, coupling, blank])
    rhs = rows([right_side[f] for f in range(4)])
    padded = (tx + 2, ty + 2)
    lanes = (tz + 2) * tile
    peers = max(counts)
    field = jax.ShapeDtypeStruct((tx, ty, 4, tz * tile), jnp.float32)
    vmem = pl.BlockSpec(memory_space=pltpu.VMEM)
    sol, res = pl.pallas_call(
        functools.partial(kernel, counts, (tx, ty, tz), tile),
        out_shape=(field, field),
        in_specs=[pl.BlockSpec(memory_space=pltpu.SMEM), vmem, vmem, vmem],
        out_specs=(vmem, vmem),
        scratch_shapes=[
            pltpu.VMEM((tx * ty * tz, 27 * tile, 2 * tile), jnp.bfloat16),
            pltpu.VMEM(padded + (8, lanes), jnp.float32),
            pltpu.VMEM(padded + (4, lanes), jnp.float32),
            pltpu.VMEM(padded + (4, lanes), jnp.float32),
            pltpu.VMEM((ITERS,) + padded + (4, lanes), jnp.float32),
            pltpu.VMEM(padded + (16, lanes), jnp.bfloat16),
            pltpu.VMEM((5, tile, tile), jnp.float32),
            pltpu.VMEM((tx, ty, 4, tz * tile), jnp.float32),
            pltpu.VMEM((tx, ty, 4, tz * tile), jnp.float32),
            pltpu.VMEM((ITERS, 3, 8, tile), jnp.float32),
            pltpu.VMEM((ITERS, 3, peers, 8, tile), jnp.float32),
            pltpu.SemaphoreType.DMA((ITERS + 1, 26)),
            pltpu.SemaphoreType.DMA((ITERS + 1, 26)),
            pltpu.SemaphoreType.DMA((ITERS, 3, peers)),
            pltpu.SemaphoreType.DMA((ITERS, 3, peers)),
        ],
        compiler_params=pltpu.CompilerParams(
            has_side_effects=True, vmem_limit_bytes=67043328
        ),
    )(pair_bits.reshape(-1), params, rhs, aux)

    def fields(x):
        return x.reshape(tx, ty, 4, tz, tile).transpose(2, 0, 1, 3, 4)

    return fields(sol), fields(res)


def solution(mesh):
    counts = tuple(mesh.shape[axis] for axis in AXES)
    tiles = P("gx", "gy", "gz", None)
    four = P(None, "gx", "gy", "gz", None)
    return jax.shard_map(
        functools.partial(on_device, counts),
        mesh=mesh,
        in_specs=(four, tiles, tiles, tiles, tiles, tiles, P("gx", "gy", "gz"), four),
        out_specs=(four, four),
        check_vma=False,
    )
```

```python
import functools
import itertools

import jax
import jax.numpy as jnp
from jax import lax
from jax.experimental import pallas as pl
from jax.experimental.pallas import tpu as pltpu
from jax.sharding import PartitionSpec as P

ITERS = 3
AXES = ("gx", "gy", "gz")
DIRECTIONS = [d for d in itertools.product((-1, 0, 1), repeat=3) if d != (0, 0, 0)]

coulomb_scale = 0.002
response_scale = 0.003


def sides(step, count, unit):
    if step < 0:
        return pl.ds(unit, unit), pl.ds((count + 1) * unit, unit)
    if step > 0:
        return pl.ds(count * unit, unit), pl.ds(0, unit)
    return pl.ds(unit, count * unit), pl.ds(unit, count * unit)


def kernel(
    counts, extent, tile,
    bits_ref, params_ref, rhs_ref, aux_ref, sol_ref, res_ref,
    store, param_pad, rem_pad, along_pad, ghosts, lhs, columns, diag, direction, sums, parts,
    halo_send, halo_recv, sum_send, sum_recv,
):
    tx, ty, tz = extent
    me = [lax.axis_index(axis) for axis in AXES]

    def exists(d):
        ok = None
        for m, step, count in zip(me, d, counts):
            if step:
                here = (m + step >= 0) & (m + step < count)
                ok = here if ok is None else ok & here
        return ok

    def halo_copy(ref, slot, index, d):
        pairs = [sides(s, n, u) for s, n, u in zip(d, extent, (1, 1, tile))]
        source = (pairs[0][0], pairs[1][0], slice(None), pairs[2][0])
        target = (pairs[0][1], pairs[1][1], slice(None), pairs[2][1])
        return pltpu.make_async_remote_copy(
            src_ref=ref.at[source],
            dst_ref=ref.at[target],
            send_sem=halo_send.at[slot, index],
            recv_sem=halo_recv.at[slot, index],
            device_id=tuple(m + s for m, s in zip(me, d)),
            device_id_type=pl.DeviceIdType.MESH,
        )

    def halo_start(ref, slot, fill):
        for index, d in enumerate(DIRECTIONS):
            there = exists(d)

            @pl.when(there)
            def _():
                halo_copy(ref, slot, index, d).start()

            back = tuple(-s for s in d)
            strips = [sides(s, n, u)[1] for s, n, u in zip(back, extent, (1, 1, tile))]

            @pl.when(jnp.logical_not(there))
            def _():
                region = (strips[0], strips[1], slice(None), strips[2])
                ref[region] = jnp.full(ref.at[region].shape, fill, jnp.float32)

    def halo_wait(ref, slot):
        for index, d in enumerate(DIRECTIONS):
            @pl.when(exists(d))
            def _():
                halo_copy(ref, slot, index, d).wait_send()

            back = tuple(-s for s in d)

            @pl.when(exists(back))
            def _():
                halo_copy(ref, slot, index, d).wait_recv()

    def sum_copies(slot, stage):
        count = counts[stage]
        copies = []
        for j in range(1, count):
            target = list(me)
            target[stage] = lax.rem(me[stage] + j, count)
            copies.append(
                pltpu.make_async_remote_copy(
                    src_ref=sums.at[slot, stage],
                    dst_ref=parts.at[slot, stage, me[stage]],
                    send_sem=sum_send.at[slot, stage, j],
                    recv_sem=sum_recv.at[slot, stage, j],
                    device_id=tuple(target),
                    device_id_type=pl.DeviceIdType.MESH,
                )
            )
        return copies

    def reduced(slot, value):
        for stage in (2, 1, 0):
            if counts[stage] == 1:
                continue
            sums[slot, stage] = value
            parts[slot, stage, me[stage]] = value
            copies = sum_copies(slot, stage)
            for copy in copies:
                copy.start()
            for copy in copies:
                copy.wait()
            value = parts[slot, stage, 0]
            for k in range(1, counts[stage]):
                value = value + parts[slot, stage, k]
        total = jnp.sum(value, axis=1, keepdims=True)
        norm, product = total[:4], total[4:]

        def both(x):
            return x + jnp.concatenate([x[2:4], x[0:2]], axis=0)

        return both(norm), both(product)

    inside = pl.ds(tile, tz * tile)
    for a in range(tx):
        for b in range(ty):
            param_pad[a + 1, b + 1, :, inside] = params_ref[a, b]
            rem_pad[a + 1, b + 1, :, inside] = rhs_ref[a, b]
    halo_start(param_pad, 0, 1.0)
    halo_start(rem_pad, 1, 0.0)

    row = lax.broadcasted_iota(jnp.int32, (8, tile), 0)

    def centred(value):
        return jnp.where(row < 3, value - 0.5, value)

    def squares(value):
        return value[0:1] * value[0:1] + value[1:2] * value[1:2] + value[2:3] * value[2:3]

    def three(value):
        first = value.astype(jnp.bfloat16).astype(jnp.float32)
        rest = value - first
        second = rest.astype(jnp.bfloat16).astype(jnp.float32)
        return first, second, rest - second

    def source_block(ap, bp, p, widths):
        start = pl.multiple_of(p * tile, tile)
        raw = param_pad[ap, bp, :, pl.ds(start, tile)]
        x = centred(raw)
        x = jnp.where(row == 4, 0.0, jnp.where(row == 5, squares(x), x))
        x = jnp.where(row == 7, 0.0, x)
        x1, x2, x3 = three(x)
        turned = jnp.concatenate([x1, x1, x1, x2, x2, x3, raw, raw], axis=0).T
        columns[...] = jnp.broadcast_to(turned[:, 52:53], (tile, tile)) * -0.6931471805599453
        partner = turned.astype(jnp.bfloat16)

        def visit(rows_of_tiles):
            for (a, b), c in itertools.product(rows_of_tiles, widths):
                o = (ap - 1 - a, bp - 1 - b, p - 1 - c)
                code = 9 * (o[0] + 1) + 3 * (o[1] + 1) + (o[2] + 1)
                t = (a * ty + b) * tz + c
                listed = jnp.right_shift(bits_ref[t], code) & 1
                own = param_pad[
                    a + 1, b + 1, :, pl.ds(pl.multiple_of((c + 1) * tile, tile), tile)
                ]
                shift = [step.astype(jnp.float32) for step in o]
                shift = jnp.where(row == 0, shift[0], jnp.where(row == 1, shift[1], shift[2]))
                r = centred(own) - shift
                y = jnp.where(row < 3, -2.0 * r, jnp.where(row == 6, squares(r), own))
                y = jnp.where((row == 4) | (row == 7), 0.0, y)
                blank = jnp.zeros((16, tile), jnp.float32)
                halves = []
                for half in (jnp.where(row == 3, 0.0, y), y):
                    y1, y2, y3 = three(half)
                    halves.append(jnp.concatenate([y1, y2, y3, y1, y2, y1, blank], axis=0))
                factors = jnp.concatenate(halves, axis=1).astype(jnp.bfloat16)
                got = jnp.dot(partner, factors, preferred_element_type=jnp.float32)
                listed = listed.astype(jnp.float32)
                coulomb = lax.rsqrt(got[:, tile:]) * (coulomb_scale * listed)
                span = columns[...] + own[4:5] * -0.6931471805599453
                response = jnp.exp2(got[:, :tile] / span) * (response_scale * listed)
                rows = pl.ds(pl.multiple_of(code * tile, tile), tile)
                store[t, rows, 0:tile] = coulomb.astype(jnp.bfloat16)
                store[t, rows, tile : 2 * tile] = response.astype(jnp.bfloat16)

        a_low, b_low = jnp.maximum(ap - 2, 0), jnp.maximum(bp - 2, 0)
        wide = jnp.minimum(bp, ty - 1) + 1 - b_low
        total = (jnp.minimum(ap, tx - 1) + 1 - a_low) * wide

        def place(n):
            return a_low + n // wide, b_low + n % wide

        def two(n, carry):
            visit([place(2 * n), place(2 * n + 1)])
            return carry

        def single(n, carry):
            visit([place(total - 1)])
            return carry

        lax.fori_loop(0, total // 2, two, 0)
        lax.fori_loop(0, total % 2, single, 0)

    def edge_sources(ap, bp, first, second, wide):
        def step(s, carry):
            p = first + s * (second - first)
            base = s * (tz - wide)
            source_block(ap, bp, p, [base + w for w in range(wide)])
            return carry

        lax.fori_loop(0, 2, step, 0)

    def middle_sources(ap, bp):
        def step(p, carry):
            source_block(ap, bp, p, [p - 2, p - 1, p])
            return carry

        lax.fori_loop(2, tz, step, 0)

    def own_rows(body):
        def over(q, carry):
            body(1 + q // ty, 1 + q % ty)
            return carry

        lax.fori_loop(0, tx * ty, over, 0)

    def build_own(ap, bp):
        middle_sources(ap, bp)
        edge_sources(ap, bp, 1, tz, 2)

    own_rows(build_own)

    same = lax.broadcasted_iota(jnp.int32, (tile, 2 * tile), 0) == (
        lax.broadcasted_iota(jnp.int32, (tile, 2 * tile), 1) % tile
    )

    def clear(t, carry):
        rows = pl.ds(13 * tile, tile)
        block = store[t, rows, :].astype(jnp.float32)
        store[t, rows, :] = jnp.where(same, 0.0, block).astype(jnp.bfloat16)
        return carry

    lax.fori_loop(0, tx * ty * tz, clear, 0)

    halo_wait(param_pad, 0)

    own_rows(lambda ap, bp: edge_sources(ap, bp, 0, tz + 1, 1))

    def ghost_row(q, carry):
        ap = q // (ty + 2)
        bp = q % (ty + 2)
        own = (ap >= 1) & (ap <= tx) & (bp >= 1) & (bp <= ty)
        held = (ap + me[0] >= 1) & (ap + me[0] <= tx + counts[0] - 1)
        held = held & (bp + me[1] >= 1) & (bp + me[1] <= ty + counts[1] - 1)

        @pl.when(jnp.logical_not(own) & held)
        def _():
            middle_sources(ap, bp)
            edge_sources(ap, bp, 1, tz, 2)
            edge_sources(ap, bp, 0, tz + 1, 1)

        @pl.when(jnp.logical_not(own) & jnp.logical_not(held))
        def _():
            def over_a(a, inner):
                def over_b(b, innermost):
                    code = 9 * (ap - a) + 3 * (bp - b)
                    rows = pl.ds(pl.multiple_of(code * tile, tile), 3 * tile)

                    def over_c(c, last):
                        store[(a * ty + b) * tz + c, rows, :] = jnp.zeros(
                            (3 * tile, 2 * tile), jnp.bfloat16
                        )
                        return last

                    return lax.fori_loop(0, tz, over_c, innermost)

                return lax.fori_loop(
                    jnp.maximum(bp - 2, 0), jnp.minimum(bp, ty - 1) + 1, over_b, inner
                )

            lax.fori_loop(jnp.maximum(ap - 2, 0), jnp.minimum(ap, tx - 1) + 1, over_a, 0)

        return carry

    lax.fori_loop(0, (tx + 2) * (ty + 2), ghost_row, 0)
    halo_wait(rem_pad, 1)

    charge_rows = lax.broadcasted_iota(jnp.int32, (4, tile), 0) < 2

    def operate(out, first):
        def split(q, carry):
            ap = q // (ty + 2)
            bp = q % (ty + 2)
            value = rem_pad[ap, bp]
            upper = value.astype(jnp.bfloat16).astype(jnp.float32)
            lower = value - upper
            ones = jnp.ones((8, value.shape[1]), jnp.float32)
            lhs[ap, bp] = jnp.concatenate([upper, lower, ones], axis=0).astype(jnp.bfloat16)
            return carry

        lax.fori_loop(0, (tx + 2) * (ty + 2), split, 0)

        def one(t, carry):
            norm, product = carry
            a = t // (ty * tz)
            b = t // tz % ty
            c = t % tz
            window = pl.ds(pl.multiple_of(c * tile, tile), 3 * tile)
            rows = jnp.concatenate(
                [lhs[a + i, b + j, :, window] for i in range(3) for j in range(3)], axis=1
            )
            got = jnp.dot(rows, store[t], preferred_element_type=jnp.float32)
            pair = got[0:4] + got[4:8]
            pair = jnp.where(charge_rows, pair[:, :tile], -pair[:, tile:])
            here = pl.ds(pl.multiple_of(c * tile, tile), tile)
            there = pl.ds(pl.multiple_of((c + 1) * tile, tile), tile)
            if first:
                row_sums = jnp.where(charge_rows, got[8:12, :tile], got[8:12, tile:])
                own = aux_ref[a, b, :, here]
                diag[a, b, :, here] = row_sums + jnp.where(charge_rows, own[0:1], own[1:2])
            vector = rem_pad[a + 1, b + 1, :, there]
            swapped = jnp.concatenate([vector[2:4], vector[0:2]], axis=0)
            link = aux_ref[a, b, 2:3, here]
            image = diag[a, b, :, here] * vector + pair + link * swapped
            out[a + 1, b + 1, :, there] = image
            return (norm + vector * vector, product + vector * image)

        zero = jnp.zeros((4, tile), jnp.float32)
        norm, product = lax.fori_loop(0, tx * ty * tz, one, (zero, zero), unroll=2)
        return jnp.concatenate([norm, product], axis=0)

    interior = (pl.ds(1, tx), pl.ds(1, ty), slice(None), inside)
    norm_now = step_size = None
    for iteration in range(ITERS):
        last = iteration + 1 == ITERS
        image = ghosts.at[iteration]
        partial = operate(image, iteration == 0)
        if not last:
            halo_start(image, 2 + iteration, 0.0)
        norm_next, product = reduced(iteration, partial)
        if not last:
            halo_wait(image, 2 + iteration)
        if iteration == 0:
            beta = None
            step_size = norm_next / product
        else:
            beta = norm_next / norm_now
            step_size = norm_next / (product - beta * norm_next / step_size)
        norm_now = norm_next
        for a in range(tx):
            for b in range(ty):
                along_dir = rem_pad[a + 1, b + 1, :, inside]
                if beta is not None:
                    along_dir = along_dir + beta * direction[a, b]
                direction[a, b] = along_dir
                moved = step_size * along_dir
                sol_ref[a, b] = moved if beta is None else sol_ref[a, b] + moved
        if last:
            for a in range(tx):
                for b in range(ty):
                    along = image[a + 1, b + 1, :, inside] + beta * along_pad[a + 1, b + 1, :, inside]
                    res_ref[a, b] = rem_pad[a + 1, b + 1, :, inside] - step_size * along
        else:
            for a in range(tx + 2):
                for b in range(ty + 2):
                    along = image[a, b]
                    if beta is not None:
                        along = along + beta * along_pad[a, b]
                    along_pad[a, b] = along
                    rem_pad[a, b] = rem_pad[a, b] - step_size * along


def on_device(counts, positions, shield, width, hardness, softness, coupling, pair_bits, right_side):
    tx, ty, tz, tile = hardness.shape
    blank = jnp.ones_like(width)

    def rows(fields):
        stacked = jnp.stack(fields, axis=2)
        return stacked.reshape(tx, ty, len(fields), tz * tile)

    params = rows([positions[0], positions[1], positions[2], shield, width, blank, blank, blank])
    aux = rows([hardness, softness, coupling, blank])
    rhs = rows([right_side[f] for f in range(4)])
    padded = (tx + 2, ty + 2)
    lanes = (tz + 2) * tile
    peers = max(counts)
    field = jax.ShapeDtypeStruct((tx, ty, 4, tz * tile), jnp.float32)
    vmem = pl.BlockSpec(memory_space=pltpu.VMEM)
    sol, res = pl.pallas_call(
        functools.partial(kernel, counts, (tx, ty, tz), tile),
        out_shape=(field, field),
        in_specs=[pl.BlockSpec(memory_space=pltpu.SMEM), vmem, vmem, vmem],
        out_specs=(vmem, vmem),
        scratch_shapes=[
            pltpu.VMEM((tx * ty * tz, 27 * tile, 2 * tile), jnp.bfloat16),
            pltpu.VMEM(padded + (8, lanes), jnp.float32),
            pltpu.VMEM(padded + (4, lanes), jnp.float32),
            pltpu.VMEM(padded + (4, lanes), jnp.float32),
            pltpu.VMEM((ITERS,) + padded + (4, lanes), jnp.float32),
            pltpu.VMEM(padded + (16, lanes), jnp.bfloat16),
            pltpu.VMEM((tile, tile), jnp.float32),
            pltpu.VMEM((tx, ty, 4, tz * tile), jnp.float32),
            pltpu.VMEM((tx, ty, 4, tz * tile), jnp.float32),
            pltpu.VMEM((ITERS, 3, 8, tile), jnp.float32),
            pltpu.VMEM((ITERS, 3, peers, 8, tile), jnp.float32),
            pltpu.SemaphoreType.DMA((ITERS + 1, 26)),
            pltpu.SemaphoreType.DMA((ITERS + 1, 26)),
            pltpu.SemaphoreType.DMA((ITERS, 3, peers)),
            pltpu.SemaphoreType.DMA((ITERS, 3, peers)),
        ],
        compiler_params=pltpu.CompilerParams(
            has_side_effects=True, vmem_limit_bytes=67043328
        ),
    )(pair_bits.reshape(-1), params, rhs, aux)

    def fields(x):
        return x.reshape(tx, ty, 4, tz, tile).transpose(2, 0, 1, 3, 4)

    return fields(sol), fields(res)


def solution(mesh):
    counts = tuple(mesh.shape[axis] for axis in AXES)
    tiles = P("gx", "gy", "gz", None)
    four = P(None, "gx", "gy", "gz", None)
    return jax.shard_map(
        functools.partial(on_device, counts),
        mesh=mesh,
        in_specs=(four, tiles, tiles, tiles, tiles, tiles, P("gx", "gy", "gz"), four),
        out_specs=(four, four),
        check_vma=False,
    )
```

```python
import functools
import itertools

import jax
import jax.numpy as jnp
from jax import lax
from jax.experimental import pallas as pl
from jax.experimental.pallas import tpu as pltpu
from jax.sharding import PartitionSpec as P

ITERS = 3
AXES = ("gx", "gy", "gz")
DIRECTIONS = [d for d in itertools.product((-1, 0, 1), repeat=3) if d != (0, 0, 0)]

coulomb_scale = 0.002
response_scale = 0.003


def sides(step, count, unit):
    if step < 0:
        return pl.ds(unit, unit), pl.ds((count + 1) * unit, unit)
    if step > 0:
        return pl.ds(count * unit, unit), pl.ds(0, unit)
    return pl.ds(unit, count * unit), pl.ds(unit, count * unit)


def kernel(
    counts, extent, tile,
    bits_ref, params_ref, rhs_ref, aux_ref, sol_ref, res_ref,
    store, param_pad, rem_pad, along_pad, ghosts, lhs, columns, diag, direction, sums, parts,
    halo_send, halo_recv, sum_send, sum_recv,
):
    tx, ty, tz = extent
    me = [lax.axis_index(axis) for axis in AXES]

    def exists(d):
        ok = None
        for m, step, count in zip(me, d, counts):
            if step:
                here = (m + step >= 0) & (m + step < count)
                ok = here if ok is None else ok & here
        return ok

    def halo_copy(ref, slot, index, d):
        pairs = [sides(s, n, u) for s, n, u in zip(d, extent, (1, 1, tile))]
        source = (pairs[0][0], pairs[1][0], slice(None), pairs[2][0])
        target = (pairs[0][1], pairs[1][1], slice(None), pairs[2][1])
        return pltpu.make_async_remote_copy(
            src_ref=ref.at[source],
            dst_ref=ref.at[target],
            send_sem=halo_send.at[slot, index],
            recv_sem=halo_recv.at[slot, index],
            device_id=tuple(m + s for m, s in zip(me, d)),
            device_id_type=pl.DeviceIdType.MESH,
        )

    def halo_start(ref, slot, fill):
        for index, d in enumerate(DIRECTIONS):
            there = exists(d)

            @pl.when(there)
            def _():
                halo_copy(ref, slot, index, d).start()

            back = tuple(-s for s in d)
            strips = [sides(s, n, u)[1] for s, n, u in zip(back, extent, (1, 1, tile))]

            @pl.when(jnp.logical_not(there))
            def _():
                region = (strips[0], strips[1], slice(None), strips[2])
                ref[region] = jnp.full(ref.at[region].shape, fill, jnp.float32)

    def halo_wait(ref, slot):
        for index, d in enumerate(DIRECTIONS):
            @pl.when(exists(d))
            def _():
                halo_copy(ref, slot, index, d).wait_send()

            back = tuple(-s for s in d)

            @pl.when(exists(back))
            def _():
                halo_copy(ref, slot, index, d).wait_recv()

    rank = (me[0] * counts[1] + me[1]) * counts[2] + me[2]
    hops = [h for h in itertools.product(*map(range, counts)) if any(h)]

    def reduced(slot, value):
        sums[slot] = value
        parts[slot, rank] = value
        copies = [
            pltpu.make_async_remote_copy(
                src_ref=sums.at[slot],
                dst_ref=parts.at[slot, rank],
                send_sem=sum_send.at[slot, j],
                recv_sem=sum_recv.at[slot, j],
                device_id=tuple(lax.rem(m + h, n) for m, h, n in zip(me, hop, counts)),
                device_id_type=pl.DeviceIdType.MESH,
            )
            for j, hop in enumerate(hops)
        ]
        for copy in copies:
            copy.start()
        for copy in copies:
            copy.wait()
        value = jnp.sum(parts[slot], axis=0)
        total = jnp.sum(value, axis=1, keepdims=True)
        norm, product = total[:4], total[4:]

        def both(x):
            return x + jnp.concatenate([x[2:4], x[0:2]], axis=0)

        return both(norm), both(product)

    inside = pl.ds(tile, tz * tile)
    for a in range(tx):
        for b in range(ty):
            param_pad[a + 1, b + 1, :, inside] = params_ref[a, b]
            rem_pad[a + 1, b + 1, :, inside] = rhs_ref[a, b]
    halo_start(param_pad, 0, 1.0)
    halo_start(rem_pad, 1, 0.0)

    row = lax.broadcasted_iota(jnp.int32, (8, tile), 0)

    def centred(value):
        return jnp.where(row < 3, value - 0.5, value)

    def squares(value):
        return value[0:1] * value[0:1] + value[1:2] * value[1:2] + value[2:3] * value[2:3]

    def three(value):
        first = value.astype(jnp.bfloat16).astype(jnp.float32)
        rest = value - first
        second = rest.astype(jnp.bfloat16).astype(jnp.float32)
        return first, second, rest - second

    def source_block(ap, bp, p, widths):
        start = pl.multiple_of(p * tile, tile)
        raw = param_pad[ap, bp, :, pl.ds(start, tile)]
        x = centred(raw)
        x = jnp.where(row == 4, 0.0, jnp.where(row == 5, squares(x), x))
        x = jnp.where(row == 7, 0.0, x)
        x1, x2, x3 = three(x)
        turned = jnp.concatenate([x1, x1, x1, x2, x2, x3, raw, raw], axis=0).T
        columns[...] = jnp.broadcast_to(turned[:, 52:53], (tile, tile)) * -0.6931471805599453
        partner = turned.astype(jnp.bfloat16)

        def visit(rows_of_tiles):
            for (a, b), c in itertools.product(rows_of_tiles, widths):
                o = (ap - 1 - a, bp - 1 - b, p - 1 - c)
                code = 9 * (o[0] + 1) + 3 * (o[1] + 1) + (o[2] + 1)
                t = (a * ty + b) * tz + c
                listed = jnp.right_shift(bits_ref[t], code) & 1
                own = param_pad[
                    a + 1, b + 1, :, pl.ds(pl.multiple_of((c + 1) * tile, tile), tile)
                ]
                shift = [step.astype(jnp.float32) for step in o]
                shift = jnp.where(row == 0, shift[0], jnp.where(row == 1, shift[1], shift[2]))
                r = centred(own) - shift
                y = jnp.where(row < 3, -2.0 * r, jnp.where(row == 6, squares(r), own))
                y = jnp.where((row == 4) | (row == 7), 0.0, y)
                blank = jnp.zeros((16, tile), jnp.float32)
                halves = []
                for half in (jnp.where(row == 3, 0.0, y), y):
                    y1, y2, y3 = three(half)
                    halves.append(jnp.concatenate([y1, y2, y3, y1, y2, y1, blank], axis=0))
                factors = jnp.concatenate(halves, axis=1).astype(jnp.bfloat16)
                got = jnp.dot(partner, factors, preferred_element_type=jnp.float32)
                listed = listed.astype(jnp.float32)
                coulomb = lax.rsqrt(got[:, tile:]) * (coulomb_scale * listed)
                span = columns[...] + own[4:5] * -0.6931471805599453
                response = jnp.exp2(got[:, :tile] / span) * (response_scale * listed)
                rows = pl.ds(pl.multiple_of(code * tile, tile), tile)
                store[t, rows, 0:tile] = coulomb.astype(jnp.bfloat16)
                store[t, rows, tile : 2 * tile] = response.astype(jnp.bfloat16)

        a_low, b_low = jnp.maximum(ap - 2, 0), jnp.maximum(bp - 2, 0)
        wide = jnp.minimum(bp, ty - 1) + 1 - b_low
        total = (jnp.minimum(ap, tx - 1) + 1 - a_low) * wide

        def place(n):
            return a_low + n // wide, b_low + n % wide

        def two(n, carry):
            visit([place(2 * n), place(2 * n + 1)])
            return carry

        def single(n, carry):
            visit([place(total - 1)])
            return carry

        lax.fori_loop(0, total // 2, two, 0)
        lax.fori_loop(0, total % 2, single, 0)

    def edge_sources(ap, bp, first, second, wide):
        def step(s, carry):
            p = first + s * (second - first)
            base = s * (tz - wide)
            source_block(ap, bp, p, [base + w for w in range(wide)])
            return carry

        lax.fori_loop(0, 2, step, 0)

    def middle_sources(ap, bp):
        def step(p, carry):
            source_block(ap, bp, p, [p - 2, p - 1, p])
            return carry

        lax.fori_loop(2, tz, step, 0)

    def own_rows(body):
        def over(q, carry):
            body(1 + q // ty, 1 + q % ty)
            return carry

        lax.fori_loop(0, tx * ty, over, 0)

    def build_own(ap, bp):
        middle_sources(ap, bp)
        edge_sources(ap, bp, 1, tz, 2)

    own_rows(build_own)

    same = lax.broadcasted_iota(jnp.int32, (tile, 2 * tile), 0) == (
        lax.broadcasted_iota(jnp.int32, (tile, 2 * tile), 1) % tile
    )

    def clear(t, carry):
        rows = pl.ds(13 * tile, tile)
        block = store[t, rows, :].astype(jnp.float32)
        store[t, rows, :] = jnp.where(same, 0.0, block).astype(jnp.bfloat16)
        return carry

    lax.fori_loop(0, tx * ty * tz, clear, 0)

    halo_wait(param_pad, 0)

    own_rows(lambda ap, bp: edge_sources(ap, bp, 0, tz + 1, 1))

    def ghost_row(q, carry):
        ap = q // (ty + 2)
        bp = q % (ty + 2)
        own = (ap >= 1) & (ap <= tx) & (bp >= 1) & (bp <= ty)
        held = (ap + me[0] >= 1) & (ap + me[0] <= tx + counts[0] - 1)
        held = held & (bp + me[1] >= 1) & (bp + me[1] <= ty + counts[1] - 1)

        @pl.when(jnp.logical_not(own) & held)
        def _():
            middle_sources(ap, bp)
            edge_sources(ap, bp, 1, tz, 2)
            edge_sources(ap, bp, 0, tz + 1, 1)

        @pl.when(jnp.logical_not(own) & jnp.logical_not(held))
        def _():
            def over_a(a, inner):
                def over_b(b, innermost):
                    code = 9 * (ap - a) + 3 * (bp - b)
                    rows = pl.ds(pl.multiple_of(code * tile, tile), 3 * tile)

                    def over_c(c, last):
                        store[(a * ty + b) * tz + c, rows, :] = jnp.zeros(
                            (3 * tile, 2 * tile), jnp.bfloat16
                        )
                        return last

                    return lax.fori_loop(0, tz, over_c, innermost)

                return lax.fori_loop(
                    jnp.maximum(bp - 2, 0), jnp.minimum(bp, ty - 1) + 1, over_b, inner
                )

            lax.fori_loop(jnp.maximum(ap - 2, 0), jnp.minimum(ap, tx - 1) + 1, over_a, 0)

        return carry

    lax.fori_loop(0, (tx + 2) * (ty + 2), ghost_row, 0)
    halo_wait(rem_pad, 1)

    charge_rows = lax.broadcasted_iota(jnp.int32, (4, tile), 0) < 2

    def operate(out, first):
        def split(q, carry):
            ap = q // (ty + 2)
            bp = q % (ty + 2)
            value = rem_pad[ap, bp]
            upper = value.astype(jnp.bfloat16).astype(jnp.float32)
            lower = value - upper
            ones = jnp.ones((8, value.shape[1]), jnp.float32)
            lhs[ap, bp] = jnp.concatenate([upper, lower, ones], axis=0).astype(jnp.bfloat16)
            return carry

        lax.fori_loop(0, (tx + 2) * (ty + 2), split, 0)

        def one(t, carry):
            norm, product = carry
            a = t // (ty * tz)
            b = t // tz % ty
            c = t % tz
            window = pl.ds(pl.multiple_of(c * tile, tile), 3 * tile)
            rows = jnp.concatenate(
                [lhs[a + i, b + j, :, window] for i in range(3) for j in range(3)], axis=1
            )
            got = jnp.dot(rows, store[t], preferred_element_type=jnp.float32)
            pair = got[0:4] + got[4:8]
            pair = jnp.where(charge_rows, pair[:, :tile], -pair[:, tile:])
            here = pl.ds(pl.multiple_of(c * tile, tile), tile)
            there = pl.ds(pl.multiple_of((c + 1) * tile, tile), tile)
            if first:
                row_sums = jnp.where(charge_rows, got[8:12, :tile], got[8:12, tile:])
                own = aux_ref[a, b, :, here]
                diag[a, b, :, here] = row_sums + jnp.where(charge_rows, own[0:1], own[1:2])
            vector = rem_pad[a + 1, b + 1, :, there]
            swapped = jnp.concatenate([vector[2:4], vector[0:2]], axis=0)
            link = aux_ref[a, b, 2:3, here]
            image = diag[a, b, :, here] * vector + pair + link * swapped
            out[a + 1, b + 1, :, there] = image
            return (norm + vector * vector, product + vector * image)

        zero = jnp.zeros((4, tile), jnp.float32)
        norm, product = lax.fori_loop(0, tx * ty * tz, one, (zero, zero), unroll=2)
        return jnp.concatenate([norm, product], axis=0)

    interior = (pl.ds(1, tx), pl.ds(1, ty), slice(None), inside)
    norm_now = step_size = None
    for iteration in range(ITERS):
        last = iteration + 1 == ITERS
        image = ghosts.at[iteration]
        partial = operate(image, iteration == 0)
        if not last:
            halo_start(image, 2 + iteration, 0.0)
        norm_next, product = reduced(iteration, partial)
        if not last:
            halo_wait(image, 2 + iteration)
        if iteration == 0:
            beta = None
            step_size = norm_next / product
        else:
            beta = norm_next / norm_now
            step_size = norm_next / (product - beta * norm_next / step_size)
        norm_now = norm_next
        for a in range(tx):
            for b in range(ty):
                along_dir = rem_pad[a + 1, b + 1, :, inside]
                if beta is not None:
                    along_dir = along_dir + beta * direction[a, b]
                direction[a, b] = along_dir
                moved = step_size * along_dir
                sol_ref[a, b] = moved if beta is None else sol_ref[a, b] + moved
        if last:
            for a in range(tx):
                for b in range(ty):
                    along = image[a + 1, b + 1, :, inside] + beta * along_pad[a + 1, b + 1, :, inside]
                    res_ref[a, b] = rem_pad[a + 1, b + 1, :, inside] - step_size * along
        else:
            for a in range(tx + 2):
                for b in range(ty + 2):
                    along = image[a, b]
                    if beta is not None:
                        along = along + beta * along_pad[a, b]
                    along_pad[a, b] = along
                    rem_pad[a, b] = rem_pad[a, b] - step_size * along


def on_device(counts, positions, shield, width, hardness, softness, coupling, pair_bits, right_side):
    tx, ty, tz, tile = hardness.shape
    blank = jnp.ones_like(width)

    def rows(fields):
        stacked = jnp.stack(fields, axis=2)
        return stacked.reshape(tx, ty, len(fields), tz * tile)

    params = rows([positions[0], positions[1], positions[2], shield, width, blank, blank, blank])
    aux = rows([hardness, softness, coupling, blank])
    rhs = rows([right_side[f] for f in range(4)])
    padded = (tx + 2, ty + 2)
    lanes = (tz + 2) * tile
    peers = counts[0] * counts[1] * counts[2]
    field = jax.ShapeDtypeStruct((tx, ty, 4, tz * tile), jnp.float32)
    vmem = pl.BlockSpec(memory_space=pltpu.VMEM)
    sol, res = pl.pallas_call(
        functools.partial(kernel, counts, (tx, ty, tz), tile),
        out_shape=(field, field),
        in_specs=[pl.BlockSpec(memory_space=pltpu.SMEM), vmem, vmem, vmem],
        out_specs=(vmem, vmem),
        scratch_shapes=[
            pltpu.VMEM((tx * ty * tz, 27 * tile, 2 * tile), jnp.bfloat16),
            pltpu.VMEM(padded + (8, lanes), jnp.float32),
            pltpu.VMEM(padded + (4, lanes), jnp.float32),
            pltpu.VMEM(padded + (4, lanes), jnp.float32),
            pltpu.VMEM((ITERS,) + padded + (4, lanes), jnp.float32),
            pltpu.VMEM(padded + (16, lanes), jnp.bfloat16),
            pltpu.VMEM((tile, tile), jnp.float32),
            pltpu.VMEM((tx, ty, 4, tz * tile), jnp.float32),
            pltpu.VMEM((tx, ty, 4, tz * tile), jnp.float32),
            pltpu.VMEM((ITERS, 8, tile), jnp.float32),
            pltpu.VMEM((ITERS, peers, 8, tile), jnp.float32),
            pltpu.SemaphoreType.DMA((ITERS + 1, 26)),
            pltpu.SemaphoreType.DMA((ITERS + 1, 26)),
            pltpu.SemaphoreType.DMA((ITERS, peers)),
            pltpu.SemaphoreType.DMA((ITERS, peers)),
        ],
        compiler_params=pltpu.CompilerParams(
            has_side_effects=True, vmem_limit_bytes=67043328
        ),
    )(pair_bits.reshape(-1), params, rhs, aux)

    def fields(x):
        return x.reshape(tx, ty, 4, tz, tile).transpose(2, 0, 1, 3, 4)

    return fields(sol), fields(res)


def solution(mesh):
    counts = tuple(mesh.shape[axis] for axis in AXES)
    tiles = P("gx", "gy", "gz", None)
    four = P(None, "gx", "gy", "gz", None)
    return jax.shard_map(
        functools.partial(on_device, counts),
        mesh=mesh,
        in_specs=(four, tiles, tiles, tiles, tiles, tiles, P("gx", "gy", "gz"), four),
        out_specs=(four, four),
        check_vma=False,
    )
```
